32 devices in a mesh: seq: 16 (over z, y, core), batch: 2 (over x).
Axes of the slice: x: 2, y: 2, z: 4, core: 2. Of those that a mesh axis runs over, the one named last changes fastest.
Arguments:
- queries: bfloat16 [4096, 1792], P(('batch', 'seq')), parts along dimension 0, may hold values from -128 to 128
- keys: bfloat16 [4096, 256], P(('batch', 'seq')), parts along dimension 0, may hold values from -4 to 4
- values: bfloat16 [4096, 256], P(('batch', 'seq')), parts along dimension 0, may hold values from -4 to 4
- out_grad: bfloat16 [4096, 1792], P(('batch', 'seq')), parts along dimension 0, may hold values from -24 to 24
- row_delta: float32 [4096, 14], P(('batch', 'seq')), parts along dimension 0, may hold values from -6 to 6
- layer_input: bfloat16 [4096, 3584], P(('batch', 'seq')), parts along dimension 0, may hold values from -6 to 6
- norm_gain: float32 [3584], replicated, may hold values from 0.25 to 1.75
- qkv_weight: bfloat16 [3584, 2304], P('seq'), may hold values from -0.5 to 0.5
- block_order: int32 [64], P('batch'), parts along dimension 0, may hold values from 0 to 31, as said below
- block_mask: int32 [64, 32], P('batch'), parts along dimension 0, may hold values from 0 to 1, as said below
- frame_owner: int32 [32], P('batch'), parts along dimension 0, may hold values from 0 to 15, as said below
- vision_features: bfloat16 [32, 128, 1152], P(('batch', 'seq')), parts along dimension 0, may hold values from -6 to 6
- post_gain: float32 [1152], replicated, may hold values from 0.25 to 1.75
- projector: bfloat16 [1152, 3584], replicated, may hold values from -0.1875 to 0.1875
Outputs:
- token_grad: bfloat16 [4096, 3584], P(('batch', 'seq')), parts along dimension 0
- encoder_grad: bfloat16 [32, 128, 1152], P(('batch', 'seq')), parts along dimension 0
The draws below stay inside these ranges and needn't reach their ends.
There are 2 independent parts, one for each index of `batch`. The reference program is written for one: setup_inputs(seed, part) draws one part's arguments, and reference() takes and returns one part's arrays. A program takes and returns all parts, laid end to end along the dimension named above; an argument that names none is the same for every part. Nothing has to cross between parts.
Inputs may be any that keep to these rules, and one draw needn't show every extreme that they name: `block_order`: entries 2i and 2i + 1 are the blocks of device i of seq; all entries together are a permutation; each device's two blocks sum to 31; for every frame f, blocks 2f and 2f + 1 lie on devices 2j and 2j + 1 for some j. `block_mask`: 1 on the diagonal, 0 above it. `frame_owner`: every device of seq owns exactly one frame, and the owner of frame f holds block 2f or block 2f + 1.
All inputs are finite; a program needn't handle non-finite values.
Results may differ from the reference program's by a relative error of at most 0.012.
Values may be sent and summed in bfloat16 or wider, within the bound.
A program may use at most 128 MiB of HBM per device.

```python
import jax
import jax.numpy as jnp
from jax import lax

D = 3584
HQ = 14
KVH = 2
HD = 128
C_ENC = 1152
TOK_DEV = 128
QKV = 2304
SEQ_LEN = 2048
FRAMES = 16
N_SEQ = 16


def frame_layout(key):
    count = N_SEQ
    groups = count // 2
    slot = jax.random.permutation(jax.random.fold_in(key, 11), groups).astype(jnp.int32)
    flip = jax.random.randint(jax.random.fold_in(key, 12), (groups,), 0, 2).astype(jnp.int32)
    order_first = jax.random.randint(jax.random.fold_in(key, 13), (groups,), 0, 2).astype(jnp.int32)
    order_second = jax.random.randint(jax.random.fold_in(key, 14), (groups,), 0, 2).astype(jnp.int32)
    owner_bit = jax.random.randint(jax.random.fold_in(key, 15), (groups,), 0, 2).astype(jnp.int32)
    group_ids = jnp.arange(groups, dtype=jnp.int32)
    device_first = (2 * slot + flip).astype(jnp.int32)
    device_second = (2 * slot + 1 - flip).astype(jnp.int32)
    first_lead = jnp.where(order_first == 1, 2 * count - 1 - 2 * group_ids, 2 * group_ids).astype(jnp.int32)
    second_lead = jnp.where(order_second == 1, 2 * count - 2 - 2 * group_ids, 2 * group_ids + 1).astype(jnp.int32)
    order = jnp.zeros((2 * count,), jnp.int32)
    order = order.at[2 * device_first].set(first_lead).at[2 * device_first + 1].set(2 * count - 1 - first_lead)
    order = order.at[2 * device_second].set(second_lead).at[2 * device_second + 1].set(2 * count - 1 - second_lead)
    owner = jnp.zeros((count,), jnp.int32)
    owner = owner.at[group_ids].set(jnp.where(owner_bit == 1, device_second, device_first))
    owner = owner.at[count - 1 - group_ids].set(jnp.where(owner_bit == 1, device_first, device_second))
    return (order.astype(jnp.int32), owner.astype(jnp.int32))


def draw_block_order(key, part):
    return frame_layout(key)[0]


def draw_frame_owner(key, part):
    return frame_layout(key)[1]


def draw_block_mask(key, part):
    count_blocks = 2 * N_SEQ
    random_bits = jax.random.randint(jax.random.fold_in(key, 21), (count_blocks, count_blocks), 0, 2).astype(jnp.int32)
    row_index = jnp.arange(count_blocks, dtype=jnp.int32)[:, None]
    column_index = jnp.arange(count_blocks, dtype=jnp.int32)[None, :]
    return jnp.where(row_index > column_index, random_bits, jnp.where(row_index == column_index, 1, 0)).astype(jnp.int32)


def attention_inputs(key):
    total_rows = TOK_DEV * N_SEQ
    half_len = TOK_DEV // 2
    group_size = HQ // KVH
    count_blocks = 2 * N_SEQ
    ranking = jnp.stack([jax.random.permutation(jax.random.fold_in(key, 40 + head), HD) for head in range(KVH)]).astype(jnp.int32)
    dim_scale = jnp.where(ranking < HD // 2, 1.5, 0.5).astype(jnp.float32)
    block_scale = jnp.exp(jax.random.uniform(jax.random.fold_in(key, 41), (count_blocks, 1, KVH, HD), jnp.float32, jnp.log(0.7), jnp.log(1.4)))
    key_scale = dim_scale[None, None, :, :] * block_scale
    limit = 4.0 / key_scale
    key_base = jax.random.truncated_normal(jax.random.fold_in(key, 31), -limit, limit, (count_blocks, half_len, KVH, HD), jnp.float32)
    keys_drawn = (key_base * key_scale).reshape(total_rows, KVH, HD)
    query_base = jax.random.truncated_normal(jax.random.fold_in(key, 32), -4.0, 4.0, (total_rows, KVH, group_size, HD), jnp.float32)
    queries_drawn = query_base * dim_scale[None, :, None, :]
    return (queries_drawn.reshape(total_rows, HQ * HD), keys_drawn.reshape(total_rows, KVH * HD))


def draw_queries(key, part):
    return attention_inputs(key)[0].astype(jnp.bfloat16)


def draw_keys(key, part):
    return attention_inputs(key)[1].astype(jnp.bfloat16)


def level_of(key, extent, cuts, smallest, largest):
    factor_of, own = 1.0, jax.random.fold_in(key, 6)
    for dim, shards_of in cuts:
        heights = jnp.exp(jax.random.uniform(jax.random.fold_in(own, dim), (shards_of,), jnp.float32, smallest / len(cuts), largest / len(cuts)))
        factor_of = factor_of * jnp.repeat(heights, extent[dim] // shards_of).reshape([-1 if axis == dim else 1 for axis in range(len(extent))])
    return factor_of


def gaussian(key, dims, scale, most, cuts=(), held_as=jnp.bfloat16):
    values = jax.random.normal(key, dims, jnp.float32) * scale
    if len(cuts) > 0:
        values = level_of(key, dims, cuts, -0.22, 0.18) * values
    return jnp.clip(values, min=-most, max=most).astype(held_as)


def setup_inputs(seed: int = 0, part: int = 0) -> dict:
    key_of = jax.random.split(jax.random.key(seed), 15)
    part_splits = jax.random.split(jax.random.fold_in(key_of[14], part), 15)
    return {
        "queries": draw_queries(jax.random.fold_in(jax.random.fold_in(key_of[14], part), 71), part),
        "keys": draw_keys(jax.random.fold_in(jax.random.fold_in(key_of[14], part), 71), part),
        "values": gaussian(part_splits[2], (SEQ_LEN, KVH * HD), 1.0, 4.0, ((0, 16),)),
        "out_grad": gaussian(part_splits[3], (SEQ_LEN, HQ * HD), 4.0, 24.0, ((0, 16),)),
        "row_delta": gaussian(part_splits[4], (SEQ_LEN, HQ), 1.0, 6.0, ((0, 16),), jnp.float32),
        "layer_input": gaussian(part_splits[5], (SEQ_LEN, D), 1.0, 6.0, ((0, 16),)),
        "norm_gain": jnp.clip(1.0 + 0.15 * jax.random.normal(key_of[6], (D,), jnp.float32), 0.25, 1.75),
        "qkv_weight": gaussian(key_of[7], (D, QKV), HD ** -0.5, 0.5, ((0, 16),)),
        "block_order": draw_block_order(jax.random.fold_in(jax.random.fold_in(key_of[14], part), 71), part),
        "block_mask": draw_block_mask(jax.random.fold_in(jax.random.fold_in(key_of[14], part), 71), part),
        "frame_owner": draw_frame_owner(jax.random.fold_in(jax.random.fold_in(key_of[14], part), 71), part),
        "vision_features": gaussian(part_splits[11], (FRAMES, TOK_DEV, C_ENC), 1.0, 6.0, ((0, 16),)),
        "post_gain": jnp.clip(1.0 + 0.15 * jax.random.normal(key_of[12], (C_ENC,), jnp.float32), 0.25, 1.75),
        "projector": gaussian(key_of[13], (C_ENC, D), C_ENC ** -0.5, 0.1875),
    }


EPSILON = 1e-06
NEGATIVE = -1e+30

def reference(queries, keys, values, out_grad, row_delta, layer_input, norm_gain, qkv_weight, block_order, block_mask, frame_owner, vision_features, post_gain, projector):
    half_len = TOK_DEV // 2
    total_rows = TOK_DEV * N_SEQ
    group_size = HQ // KVH
    scaling = HD ** (-0.5)
    row_ids = jnp.arange(total_rows, dtype=jnp.int32)
    position = (block_order[row_ids // half_len] * half_len + row_ids % half_len).astype(jnp.int32)
    blocks = (position // half_len).astype(jnp.int32)
    query_heads = queries.reshape(total_rows, HQ, HD)
    grad_heads = out_grad.reshape(total_rows, HQ, HD)
    key_heads = keys.reshape(total_rows, KVH, HD)
    value_heads = values.reshape(total_rows, KVH, HD)

    def one_head(head_index):
        kv_index = (head_index // group_size).astype(jnp.int32)
        query_rows = lax.dynamic_index_in_dim(query_heads, head_index, 1, keepdims=False)
        grad_rows = lax.dynamic_index_in_dim(grad_heads, head_index, 1, keepdims=False)
        key_rows = lax.dynamic_index_in_dim(key_heads, kv_index, 1, keepdims=False)
        value_rows = lax.dynamic_index_in_dim(value_heads, kv_index, 1, keepdims=False)
        delta_rows = lax.dynamic_index_in_dim(row_delta, head_index, 1, keepdims=False)

        def per_block(running, block_start):
            key_acc, value_acc = running
            query_block = lax.dynamic_slice_in_dim(query_rows, block_start, TOK_DEV, 0)
            grad_block = lax.dynamic_slice_in_dim(grad_rows, block_start, TOK_DEV, 0)
            delta_block = lax.dynamic_slice_in_dim(delta_rows, block_start, TOK_DEV, 0)
            pos_block = lax.dynamic_slice_in_dim(position, block_start, TOK_DEV, 0)
            block_ids = lax.dynamic_slice_in_dim(blocks, block_start, TOK_DEV, 0)
            allowed = (block_mask[block_ids][:, blocks] == 1) & (position[None, :] <= pos_block[:, None])
            score = jnp.dot(query_block, key_rows.T, preferred_element_type=jnp.float32) * scaling
            top_score = lax.optimization_barrier(jnp.max(jnp.where(allowed, score, NEGATIVE), axis=1))
            total_exp = lax.optimization_barrier(jnp.sum(jnp.where(allowed, jnp.exp(score - top_score[:, None]), 0.0), axis=1))
            lse = top_score + jnp.log(total_exp)
            prob = jnp.where(allowed, jnp.exp(score - lse[:, None]), 0.0)
            prob_low = prob.astype(jnp.bfloat16)
            value_acc = value_acc + jnp.dot(prob_low.T, grad_block, preferred_element_type=jnp.float32)
            prob_grad = jnp.dot(grad_block, value_rows.T, preferred_element_type=jnp.float32)
            score_grad = (prob * (prob_grad - delta_block[:, None])).astype(jnp.bfloat16)
            query_out = jnp.dot(score_grad, key_rows, preferred_element_type=jnp.float32) * scaling
            key_acc = key_acc + jnp.dot(score_grad.T, query_block, preferred_element_type=jnp.float32)
            return ((key_acc, value_acc), query_out)
        starting = (jnp.zeros((total_rows, HD), jnp.float32), jnp.zeros((total_rows, HD), jnp.float32))
        starts = (jnp.arange(N_SEQ, dtype=jnp.int32) * TOK_DEV).astype(jnp.int32)
        finals, query_parts = lax.scan(per_block, starting, starts)
        return (query_parts.reshape(total_rows, HD), finals[0] * scaling, finals[1])
    query_all, key_all, value_all = lax.map(one_head, jnp.arange(HQ, dtype=jnp.int32))
    query_grad = jnp.transpose(query_all, (1, 0, 2)).reshape(total_rows, HQ * HD)
    key_grad = jnp.transpose(lax.optimization_barrier(jnp.sum(key_all.reshape(KVH, group_size, total_rows, HD), axis=1)), (1, 0, 2)).reshape(total_rows, KVH * HD)
    value_grad = jnp.transpose(lax.optimization_barrier(jnp.sum(value_all.reshape(KVH, group_size, total_rows, HD), axis=1)), (1, 0, 2)).reshape(total_rows, KVH * HD)
    head_grads = jnp.concatenate([query_grad, key_grad, value_grad], axis=1).astype(jnp.bfloat16)
    norm_grad = jnp.dot(head_grads, qkv_weight.T, preferred_element_type=jnp.float32).astype(jnp.bfloat16)
    inputs = layer_input.astype(jnp.float32)
    inverse = lax.rsqrt(lax.optimization_barrier(jnp.mean(inputs * inputs, axis=1, keepdims=True)) + EPSILON)
    scaled = norm_grad.astype(jnp.float32) * norm_gain
    token_grad = (inverse * scaled - inputs * inverse ** 3 * lax.optimization_barrier(jnp.mean(scaled * inputs, axis=1, keepdims=True))).astype(jnp.bfloat16)
    row_of_position = jnp.zeros((total_rows,), jnp.int32).at[position].set(row_ids)
    device_ids = jnp.arange(N_SEQ, dtype=jnp.int32)
    frame_of_device = jnp.zeros((N_SEQ,), jnp.int32).at[frame_owner].set(device_ids)
    spatial = jnp.arange(TOK_DEV, dtype=jnp.int32)
    frame_rows = row_of_position[(frame_of_device[:, None] * TOK_DEV + spatial[None, :]).astype(jnp.int32)]
    frame_grad = token_grad[frame_rows]
    post_grad = jnp.dot(frame_grad.reshape(N_SEQ * TOK_DEV, D), projector.T, preferred_element_type=jnp.float32).reshape(N_SEQ, TOK_DEV, C_ENC)
    features = vision_features.astype(jnp.float32)
    centered = features - lax.optimization_barrier(jnp.mean(features, axis=2, keepdims=True))
    deviation = lax.rsqrt(lax.optimization_barrier(jnp.mean(centered * centered, axis=2, keepdims=True)) + EPSILON)
    normed = centered * deviation
    weighted = post_grad * post_gain
    encoder_grad = (deviation * (weighted - lax.optimization_barrier(jnp.mean(weighted, axis=2, keepdims=True)) - normed * lax.optimization_barrier(jnp.mean(weighted * normed, axis=2, keepdims=True)))).astype(jnp.bfloat16)
    return (token_grad, encoder_grad)
```

```python
import functools

import jax
import jax.numpy as jnp
from jax import lax
from jax.experimental import pallas as pl
from jax.experimental.pallas import tpu as pltpu
from jax.sharding import PartitionSpec as P

HQ = 14
KVH = 2
HD = 128
GROUP = HQ // KVH
CHUNK = 4
LOG2E = 1.4426950408889634


EPSILON = 1e-06
NEGATIVE = -1e30


def attention_kernel(
    order_ref,
    mask_ref,
    q_ref,
    do_ref,
    delta_ref,
    kv_ref,
    dq_ref,
    dkv_ref,
    slots,
    scores,
    dq_acc,
    acc,
):
    me = lax.axis_index("seq")
    blocks = order_ref.shape[0]
    half = q_ref.shape[0] // 2
    lanes = delta_ref.shape[2]
    tall = CHUNK * half
    scaling = HD ** (-0.5)
    factor = scaling * LOG2E
    width = KVH * HD
    acc[...] = jnp.zeros_like(acc)

    row = lax.broadcasted_iota(jnp.int32, (tall, lanes), 0)
    query_at = lax.rem(lax.broadcasted_iota(jnp.int32, (tall, lanes), 1), half)
    ahead = (row < half) & (row > query_at)

    for b in range(2):
        own = 2 * me + b
        query_block = order_ref[own]
        slots[0] = own

        def collect(slot, count):
            key_block = order_ref[slot]
            live = (mask_ref[query_block, key_block] == 1) & (key_block < query_block)
            slots[count] = slot
            return count + live.astype(jnp.int32)

        count = lax.fori_loop(0, blocks, collect, jnp.int32(1))
        for extra in range(CHUNK):
            slots[count + extra] = own
        chunks = (count + CHUNK - 1) // CHUNK

        for g in range(KVH):
            pad = jnp.zeros((lanes - GROUP * half, HD), jnp.bfloat16)

            def stacked(ref):
                parts = [
                    ref[b * half : (b + 1) * half, h * HD : (h + 1) * HD]
                    for h in range(g * GROUP, (g + 1) * GROUP)
                ]
                return jnp.concatenate(parts + [pad], axis=0)

            queries = stacked(q_ref)
            grads = stacked(do_ref)
            delta = delta_ref[2 * g + b]

            def key_rows(chunk, first_col):
                parts = [
                    kv_ref[
                        pl.ds(pl.multiple_of(slots[chunk * CHUNK + i] * half, half), half),
                        first_col : first_col + HD,
                    ]
                    for i in range(CHUNK)
                ]
                return jnp.concatenate(parts, axis=0)

            def score_pass(chunk, top):
                keys = key_rows(chunk, g * HD)
                score = lax.dot_general(
                    keys, queries, (((1,), (1,)), ((), ())), preferred_element_type=jnp.float32
                )
                limit = jnp.minimum((count - chunk * CHUNK) * half, tall)
                dead = (row >= limit) | (ahead & (chunk == 0))
                score = jnp.where(dead, NEGATIVE, score)
                scores[chunk] = score
                return jnp.maximum(top, jnp.max(score.reshape(tall // 8, 8, lanes), axis=0))

            top = lax.fori_loop(
                0, chunks, score_pass, jnp.full((8, lanes), NEGATIVE, jnp.float32)
            )
            top = jnp.max(top, axis=0, keepdims=True)

            def exp_pass(chunk, total):
                spread = jnp.exp2((scores[chunk] - top) * factor)
                scores[chunk] = spread
                return total + jnp.sum(spread.reshape(tall // 8, 8, lanes), axis=0)

            total = lax.fori_loop(0, chunks, exp_pass, jnp.zeros((8, lanes), jnp.float32))
            inverse = 1.0 / jnp.sum(total, axis=0, keepdims=True)
            dq_acc[...] = jnp.zeros_like(dq_acc)

            def grad_pass(chunk, carry):
                keys = key_rows(chunk, g * HD)
                vals = key_rows(chunk, width + g * HD)
                prob = scores[chunk] * inverse
                value_add = jnp.dot(
                    prob.astype(jnp.bfloat16), grads, preferred_element_type=jnp.float32
                )
                prob_grad = lax.dot_general(
                    vals, grads, (((1,), (1,)), ((), ())), preferred_element_type=jnp.float32
                )
                score_grad = (prob * (prob_grad - delta)).astype(jnp.bfloat16)
                key_add = (
                    jnp.dot(score_grad, queries, preferred_element_type=jnp.float32) * scaling
                )
                dq_acc[...] += lax.dot_general(
                    keys, score_grad, (((0,), (0,)), ((), ())), preferred_element_type=jnp.float32
                )
                for i in range(CHUNK):
                    here = pl.ds(pl.multiple_of(slots[chunk * CHUNK + i] * half, half), half)
                    part = slice(i * half, (i + 1) * half)
                    acc[here, g * HD : (g + 1) * HD] += key_add[part]
                    acc[here, width + g * HD : width + (g + 1) * HD] += value_add[part]
                return carry

            lax.fori_loop(0, chunks, grad_pass, 0)
            turned = (jnp.transpose(dq_acc[...]) * scaling).astype(jnp.bfloat16)
            for j in range(GROUP):
                h = g * GROUP + j
                dq_ref[b * half : (b + 1) * half, h * HD : (h + 1) * HD] = turned[
                    j * half : (j + 1) * half
                ]
    dkv_ref[...] = acc[...].astype(dkv_ref.dtype)


def attention_grads(order, mask, queries, out_grad, row_delta, kv):
    rows = queries.shape[0]
    half = rows // 2
    keys = kv.shape[0]
    lanes = -(-GROUP * half // 128) * 128
    blocks = order.shape[0]
    delta = jnp.transpose(row_delta.reshape(2, half, KVH, GROUP), (2, 0, 3, 1))
    delta = delta.reshape(2 * KVH, 1, GROUP * half)
    delta = jnp.pad(delta, ((0, 0), (0, 0), (0, lanes - GROUP * half)))
    max_chunks = -(-blocks // CHUNK)
    smem = pl.BlockSpec(memory_space=pltpu.SMEM)
    vmem = pl.BlockSpec(memory_space=pltpu.VMEM)
    return pl.pallas_call(
        attention_kernel,
        out_shape=(
            jax.ShapeDtypeStruct((rows, HQ * HD), jnp.bfloat16),
            jax.ShapeDtypeStruct((keys, 2 * KVH * HD), jnp.bfloat16),
        ),
        in_specs=[smem, smem, vmem, vmem, vmem, vmem],
        out_specs=(vmem, vmem),
        scratch_shapes=[
            pltpu.SMEM((blocks + CHUNK + 1,), jnp.int32),
            pltpu.VMEM((max_chunks, CHUNK * half, lanes), jnp.float32),
            pltpu.VMEM((HD, lanes), jnp.float32),
            pltpu.VMEM((keys, 2 * KVH * HD), jnp.float32),
        ],
        cost_estimate=pl.CostEstimate(
            flops=5 * rows * keys * HQ * HD,
            bytes_accessed=4 * keys * KVH * HD * 2 + 3 * rows * HQ * HD * 2,
            transcendentals=rows * keys * HQ // 2,
        ),
        compiler_params=pltpu.CompilerParams(vmem_limit_bytes=48 * 1024 * 1024),
        name="attention_grads",
    )(order, mask, queries, out_grad, delta, kv)


def shifted(value, axis, steps):
    count = lax.axis_size(axis)
    pairs = [(source, (source + steps) % count) for source in range(count)]
    return lax.ppermute(value, axis, pairs)


def swapped(array, axis, apart):
    return lax.ppermute(array, axis, [(i, i ^ 1 << apart) for i in range(lax.axis_size(axis))])


def body(
    queries,
    keys,
    values,
    out_grad,
    row_delta,
    layer_input,
    norm_gain,
    qkv_weight,
    block_order,
    block_mask,
    frame_owner,
    vision_features,
    post_gain,
    projector,
):
    tok_rows = queries.shape[0]
    half_len = tok_rows // 2
    my_index = lax.axis_index("seq")
    my_blocks = lax.dynamic_slice_in_dim(block_order, 2 * my_index, 2, 0)
    kv = lax.all_gather(jnp.concatenate([keys, values], axis=1), "seq", axis=0, tiled=True)
    query_grad, kv_part = attention_grads(
        block_order, block_mask, queries, out_grad, row_delta, kv
    )
    kv_grad = lax.psum_scatter(kv_part, "seq", scatter_dimension=0, tiled=True)
    head_grads = jnp.concatenate([query_grad, kv_grad], axis=1)
    norm_grad = jnp.dot(
        head_grads,
        lax.all_gather(qkv_weight, "seq", axis=0, tiled=True).T,
        preferred_element_type=jnp.float32,
    ).astype(jnp.bfloat16)
    inputs = layer_input.astype(jnp.float32)
    inverse = lax.rsqrt(jnp.mean(inputs * inputs, axis=1, keepdims=True) + EPSILON)
    scaled = norm_grad.astype(jnp.float32) * norm_gain
    token_grad = (
        inverse * scaled - inputs * inverse**3 * jnp.mean(scaled * inputs, axis=1, keepdims=True)
    ).astype(jnp.bfloat16)
    frame_table = jnp.arange(frame_owner.shape[0], dtype=jnp.int32)
    my_frame = jnp.sum(jnp.where(frame_owner == my_index, frame_table, 0))
    keep_first = my_blocks[0] // 2 == my_frame
    kept_block = jnp.where(keep_first, my_blocks[0], my_blocks[1])
    leading = kept_block % 2 == 0
    halves = token_grad.reshape(2, half_len, token_grad.shape[1])
    kept = jnp.where(keep_first, halves[0], halves[1])
    sending = jnp.where(keep_first, halves[1], halves[0])
    received = swapped(sending, "seq", 0)
    frame_rows = jnp.where(
        leading,
        jnp.concatenate([kept, received], axis=0),
        jnp.concatenate([received, kept], axis=0),
    )
    post_grad = jnp.dot(frame_rows, projector.T, preferred_element_type=jnp.float32)
    features = vision_features[0].astype(jnp.float32)
    centered = features - jnp.mean(features, axis=1, keepdims=True)
    deviation = lax.rsqrt(jnp.mean(centered * centered, axis=1, keepdims=True) + EPSILON)
    normed = centered * deviation
    weighted = post_grad * post_gain
    encoder_grad = (
        deviation
        * (
            weighted
            - jnp.mean(weighted, axis=1, keepdims=True)
            - normed * jnp.mean(weighted * normed, axis=1, keepdims=True)
        )
    ).astype(jnp.bfloat16)
    return (token_grad, encoder_grad[None])


def solution(mesh):
    placed = (
        P(("batch", "seq"), None),
        P(("batch", "seq"), None),
        P(("batch", "seq"), None),
        P(("batch", "seq"), None),
        P(("batch", "seq"), None),
        P(("batch", "seq"), None),
        P(),
        P("seq", None),
        P("batch"),
        P("batch", None),
        P("batch"),
        P(("batch", "seq"), None, None),
        P(),
        P(),
    )
    return jax.shard_map(
        body,
        mesh=mesh,
        in_specs=placed,
        out_specs=(P(("batch", "seq"), None), P(("batch", "seq"), None, None)),
        check_vma=False,
    )
```

```python
import functools

import jax
import jax.numpy as jnp
from jax import lax
from jax.experimental import pallas as pl
from jax.experimental.pallas import tpu as pltpu
from jax.sharding import PartitionSpec as P

HQ = 14
KVH = 2
HD = 128
GROUP = HQ // KVH
CHUNK = 4
LOG2E = 1.4426950408889634


EPSILON = 1e-06
NEGATIVE = -1e30


def attention_kernel(
    order_ref,
    mask_ref,
    q_ref,
    do_ref,
    delta_ref,
    kv_ref,
    dq_ref,
    dkv_ref,
    slots,
    scores,
    dq_acc,
    acc,
):
    me = lax.axis_index("seq")
    blocks = order_ref.shape[0]
    half = q_ref.shape[0] // 2
    lanes = delta_ref.shape[2]
    tall = CHUNK * half
    scaling = HD ** (-0.5)
    factor = scaling * LOG2E
    width = KVH * HD
    acc[...] = jnp.zeros_like(acc)

    row = lax.broadcasted_iota(jnp.int32, (tall, lanes), 0)
    query_at = lax.rem(lax.broadcasted_iota(jnp.int32, (tall, lanes), 1), half)
    ahead = (row < half) & (row > query_at)

    for b in range(2):
        own = 2 * me + b
        query_block = order_ref[own]
        slots[0] = own

        def collect(slot, count):
            key_block = order_ref[slot]
            live = (mask_ref[query_block, key_block] == 1) & (key_block < query_block)
            slots[count] = slot
            return count + live.astype(jnp.int32)

        count = lax.fori_loop(0, blocks, collect, jnp.int32(1))
        for extra in range(CHUNK):
            slots[count + extra] = own
        chunks = (count + CHUNK - 1) // CHUNK

        for g in range(KVH):
            pad = jnp.zeros((lanes - GROUP * half, HD), jnp.bfloat16)

            def stacked(ref):
                parts = [
                    ref[b * half : (b + 1) * half, h * HD : (h + 1) * HD]
                    for h in range(g * GROUP, (g + 1) * GROUP)
                ]
                return jnp.concatenate(parts + [pad], axis=0)

            queries = stacked(q_ref)
            grads = stacked(do_ref)
            delta = delta_ref[2 * g + b]

            def key_rows(chunk, first_col):
                parts = [
                    kv_ref[
                        pl.ds(pl.multiple_of(slots[chunk * CHUNK + i] * half, half), half),
                        first_col : first_col + HD,
                    ]
                    for i in range(CHUNK)
                ]
                return jnp.concatenate(parts, axis=0)

            def score_pass(chunk, top):
                keys = key_rows(chunk, g * HD)
                score = lax.dot_general(
                    keys, queries, (((1,), (1,)), ((), ())), preferred_element_type=jnp.float32
                )
                limit = jnp.minimum((count - chunk * CHUNK) * half, tall)
                dead = (row >= limit) | (ahead & (chunk == 0))
                score = jnp.where(dead, NEGATIVE, score)
                scores[chunk] = score
                return jnp.maximum(top, jnp.max(score.reshape(tall // 8, 8, lanes), axis=0))

            top = lax.fori_loop(
                0, chunks, score_pass, jnp.full((8, lanes), NEGATIVE, jnp.float32)
            )
            top = jnp.max(top, axis=0, keepdims=True)

            def exp_pass(chunk, total):
                spread = jnp.exp2((scores[chunk] - top) * factor)
                scores[chunk] = spread
                return total + jnp.sum(spread.reshape(tall // 8, 8, lanes), axis=0)

            total = lax.fori_loop(0, chunks, exp_pass, jnp.zeros((8, lanes), jnp.float32))
            inverse = 1.0 / jnp.sum(total, axis=0, keepdims=True)
            dq_acc[...] = jnp.zeros_like(dq_acc)

            def grad_pass(chunk, carry):
                keys = key_rows(chunk, g * HD)
                vals = key_rows(chunk, width + g * HD)
                prob = scores[chunk] * inverse
                value_add = jnp.dot(
                    prob.astype(jnp.bfloat16), grads, preferred_element_type=jnp.float32
                )
                prob_grad = lax.dot_general(
                    vals, grads, (((1,), (1,)), ((), ())), preferred_element_type=jnp.float32
                )
                score_grad = (prob * (prob_grad - delta)).astype(jnp.bfloat16)
                key_add = (
                    jnp.dot(score_grad, queries, preferred_element_type=jnp.float32) * scaling
                )
                dq_acc[...] += lax.dot_general(
                    keys, score_grad, (((0,), (0,)), ((), ())), preferred_element_type=jnp.float32
                )
                for i in range(CHUNK):
                    here = pl.ds(pl.multiple_of(slots[chunk * CHUNK + i] * half, half), half)
                    part = slice(i * half, (i + 1) * half)
                    acc[here, g * HD : (g + 1) * HD] += key_add[part]
                    acc[here, width + g * HD : width + (g + 1) * HD] += value_add[part]
                return carry

            lax.fori_loop(0, chunks, grad_pass, 0)
            turned = (jnp.transpose(dq_acc[...]) * scaling).astype(jnp.bfloat16)
            for j in range(GROUP):
                h = g * GROUP + j
                dq_ref[b * half : (b + 1) * half, h * HD : (h + 1) * HD] = turned[
                    j * half : (j + 1) * half
                ]
    dkv_ref[...] = acc[...].astype(dkv_ref.dtype)


def attention_grads(order, mask, queries, out_grad, row_delta, kv):
    rows = queries.shape[0]
    half = rows // 2
    keys = kv.shape[0]
    lanes = -(-GROUP * half // 128) * 128
    blocks = order.shape[0]
    delta = jnp.transpose(row_delta.reshape(2, half, KVH, GROUP), (2, 0, 3, 1))
    delta = delta.reshape(2 * KVH, 1, GROUP * half)
    delta = jnp.pad(delta, ((0, 0), (0, 0), (0, lanes - GROUP * half)))
    max_chunks = -(-blocks // CHUNK)
    smem = pl.BlockSpec(memory_space=pltpu.SMEM)
    vmem = pl.BlockSpec(memory_space=pltpu.VMEM)
    return pl.pallas_call(
        attention_kernel,
        out_shape=(
            jax.ShapeDtypeStruct((rows, HQ * HD), jnp.bfloat16),
            jax.ShapeDtypeStruct((keys, 2 * KVH * HD), jnp.bfloat16),
        ),
        in_specs=[smem, smem, vmem, vmem, vmem, vmem],
        out_specs=(vmem, vmem),
        scratch_shapes=[
            pltpu.SMEM((blocks + CHUNK + 1,), jnp.int32),
            pltpu.VMEM((max_chunks, CHUNK * half, lanes), jnp.float32),
            pltpu.VMEM((HD, lanes), jnp.float32),
            pltpu.VMEM((keys, 2 * KVH * HD), jnp.float32),
        ],
        cost_estimate=pl.CostEstimate(
            flops=5 * rows * keys * HQ * HD,
            bytes_accessed=4 * keys * KVH * HD * 2 + 3 * rows * HQ * HD * 2,
            transcendentals=rows * keys * HQ // 2,
        ),
        compiler_params=pltpu.CompilerParams(vmem_limit_bytes=48 * 1024 * 1024),
        name="attention_grads",
    )(order, mask, queries, out_grad, delta, kv)


MESH = pl.DeviceIdType.MESH


def remote(src, dst, send_sem, recv_sem, device):
    return pltpu.make_async_remote_copy(
        src_ref=src,
        dst_ref=dst,
        send_sem=send_sem,
        recv_sem=recv_sem,
        device_id=device,
        device_id_type=MESH,
    )


def when(condition, action):
    if condition is None:
        action()
    else:
        pl.when(condition)(action)


def places():
    me = lax.axis_index("seq")
    x = lax.rem(lax.axis_index("batch"), 2)
    z, y, c = me // 4, lax.rem(me // 2, 2), lax.rem(me, 2)
    return me, x, z, y, c


def gather_kernel(
    depth,
    kv_ref,
    w_ref,
    kv_all,
    w_all,
    own_sem,
    kv_recv,
    kv_core_recv,
    kv_up,
    kv_down,
    kv_y,
    kv_core,
    w_recv,
    w_x_recv,
    w_core_recv,
    w_cx_recv,
    w_up,
    w_down,
    w_y,
    w_x,
    w_core,
    w_cx,
):
    me, x, z, y, c = places()
    rows = w_ref.shape[0]
    part = 5 * (rows // 16) // 14 * 16
    up, down = {"seq": me + 4}, {"seq": me - 4}
    beside, core = {"seq": me + 2 - 4 * y}, {"seq": me + 1 - 2 * c}
    across = {"batch": lax.axis_index("batch") + 1 - 2 * x}
    has_up, has_down = z < depth - 1, z > 0

    barrier = pltpu.get_barrier_semaphore()
    for peer, present in (
        (up, has_up),
        (down, has_down),
        (beside, None),
        (core, None),
        (across, None),
    ):
        when(
            present,
            lambda peer=peer: pl.semaphore_signal(
                barrier, inc=1, device_id=peer, device_id_type=MESH
            ),
        )
    pl.semaphore_wait(barrier, 3 + has_up.astype(jnp.int32) + has_down.astype(jnp.int32))

    started = []

    def start(copy, condition=None):
        when(condition, copy.start)
        started.append((condition, copy))

    def both(first, second):
        return second if first is None else jnp.logical_and(first, second)

    def line(step):
        if step == 0:
            return [(z, None, None)]
        return [(z - step, z - step >= 0, True), (z + step, z + step < depth, False)]

    def slot(j, side):
        return 2 * j + side

    own_kv = pltpu.make_async_copy(kv_ref, kv_all.at[me], own_sem.at[0])
    own_w = pltpu.make_async_copy(w_ref, w_all.at[me], own_sem.at[1])

    def kv_at(u):
        return kv_all.at[2 * u + c]

    def kv_pass(j, condition, upward, first):
        u = slot(j, y)
        src = kv_ref if first else kv_at(u)
        if upward is not False:
            start(remote(src, kv_at(u), kv_up.at[j], kv_recv.at[u], up), both(condition, has_up))
        if upward is not True:
            start(
                remote(src, kv_at(u), kv_down.at[j], kv_recv.at[u], down),
                both(condition, has_down),
            )
        start(remote(src, kv_at(u), kv_y.at[j], kv_recv.at[u], beside), condition)
        start(remote(src, kv_at(u), kv_core.at[u], kv_core_recv.at[u], core), condition)

    def arrived(ref, semaphore, condition=None):
        when(condition, remote(ref, ref, own_sem.at[2], semaphore, core).wait_recv)

    def safe(j):
        return jnp.clip(j, 0, depth - 1)

    kv_pass(z, None, None, True)
    own_kv.start()
    own_w.start()
    for step in range(1, depth):
        for j, condition, upward in line(step):
            j = safe(j)
            arrived(kv_at(slot(j, y)), kv_recv.at[slot(j, y)], condition)
            kv_pass(j, condition, upward, False)

    main = pl.ds(pl.multiple_of(x * part, 16), rows - part)
    mine = pl.ds(pl.multiple_of(x * (rows - part), 16), part)
    other = pl.ds(pl.multiple_of((1 - x) * (rows - part), 16), part)

    def w_at(u, which):
        return w_all.at[2 * u + c, which]

    def w_pass(j, condition, upward, first):
        u = slot(j, y)
        src = w_ref.at[main] if first else w_at(u, main)
        dst = w_at(u, main)
        if upward is not False:
            start(remote(src, dst, w_up.at[j], w_recv.at[u], up), both(condition, has_up))
        if upward is not True:
            start(remote(src, dst, w_down.at[j], w_recv.at[u], down), both(condition, has_down))
        start(remote(src, dst, w_y.at[j], w_recv.at[u], beside), condition)

    def w_share(u, condition):
        start(
            remote(w_at(u, mine), w_at(u, mine), w_x.at[u], w_x_recv.at[u], across), condition
        )
        start(
            remote(w_at(u, main), w_at(u, main), w_core.at[u], w_core_recv.at[u], core), condition
        )

    def w_finish(u, condition):
        arrived(w_at(u, other), w_x_recv.at[u], condition)
        start(
            remote(w_at(u, other), w_at(u, other), w_cx.at[u], w_cx_recv.at[u], core), condition
        )

    w_pass(z, None, None, True)
    own_u = slot(z, y)
    start(
        remote(w_ref.at[main], w_at(own_u, main), w_core.at[own_u], w_core_recv.at[own_u], core)
    )
    start(remote(w_ref.at[other], w_at(own_u, other), w_cx.at[own_u], w_cx_recv.at[own_u], core))

    for step in range(depth):
        for j, condition, _ in line(step):
            u = slot(safe(j), 1 - y)
            arrived(kv_at(u), kv_recv.at[u], condition)
            start(remote(kv_at(u), kv_at(u), kv_core.at[u], kv_core_recv.at[u], core), condition)

    waiting = []
    for step in range(1, depth + 1):
        shared = []
        if step < depth:
            for j, condition, upward in line(step):
                j = safe(j)
                u = slot(j, y)
                arrived(w_at(u, main), w_recv.at[u], condition)
                w_pass(j, condition, upward, False)
                w_share(u, condition)
                shared.append((u, condition))
        for j, condition, _ in line(step - 1):
            u = slot(safe(j), 1 - y)
            arrived(w_at(u, main), w_recv.at[u], condition)
            w_share(u, condition)
            shared.append((u, condition))
        for u, condition in waiting:
            w_finish(u, condition)
        waiting = shared
    for u, condition in waiting:
        w_finish(u, condition)

    for u in range(2 * depth):
        from_core = 2 * u + 1 - c
        arrived(kv_all.at[from_core], kv_core_recv.at[u])
        arrived(w_all.at[from_core, main], w_core_recv.at[u])
        arrived(w_all.at[from_core, other], w_cx_recv.at[u])
    for condition, copy in started:
        when(condition, copy.wait_send)
    own_kv.wait()
    own_w.wait()


def gather(kv, weight, count):
    depth = count // 4
    line, pairs = pltpu.SemaphoreType.DMA((depth,)), pltpu.SemaphoreType.DMA((2 * depth,))
    anywhere = pl.BlockSpec(memory_space=pl.ANY)
    vmem = pl.BlockSpec(memory_space=pltpu.VMEM)
    return pl.pallas_call(
        functools.partial(gather_kernel, depth),
        out_shape=(
            jax.ShapeDtypeStruct((count,) + kv.shape, kv.dtype),
            jax.ShapeDtypeStruct((count,) + weight.shape, weight.dtype),
        ),
        in_specs=[vmem, vmem],
        out_specs=(anywhere, anywhere),
        scratch_shapes=[pltpu.SemaphoreType.DMA((3,))]
        + [pairs, pairs, line, line, line, pairs]
        + [pairs, pairs, pairs, pairs, line, line, line, pairs, pairs, pairs],
        compiler_params=pltpu.CompilerParams(collective_id=0, has_side_effects=True),
        name="gather",
    )(kv, weight)


def reduce_kernel(
    depth,
    part_ref,
    out_ref,
    core_in,
    sum_out,
    y_in,
    z_in,
    core_send,
    core_recv,
    y_send,
    y_recv,
    z_send,
    z_recv,
):
    me, x, z, y, c = places()
    beside, core = {"seq": me + 2 - 4 * y}, {"seq": me + 1 - 2 * c}

    def far(k):
        return lax.rem(z + k, depth)

    barrier = pltpu.get_barrier_semaphore()
    peers = [beside, core] + [{"seq": 4 * far(k) + 2 * y + c} for k in range(1, depth)]
    for peer in peers:
        pl.semaphore_signal(barrier, inc=1, device_id=peer, device_id_type=MESH)
    pl.semaphore_wait(barrier, len(peers))

    def wide(ref):
        return ref[...].astype(jnp.float32)

    order = list(range(1, depth)) + [0]
    started = []

    def start(copy):
        copy.start()
        started.append(copy)

    core_copies, y_copies = {}, {}
    for side in (1, 0):
        for k in order:
            u = 2 * far(k) + (y if side == 0 else 1 - y)
            copy = remote(
                part_ref.at[2 * u + 1 - c], core_in.at[u], core_send.at[u], core_recv.at[u], core
            )
            start(copy)
            core_copies[side, k] = (copy, u)

    def arrived(ref, send_semaphore, semaphore, device):
        remote(ref, ref, send_semaphore, semaphore, device).wait_recv()

    for k in order:
        j = far(k)
        u = 2 * j + 1 - y
        arrived(core_in.at[u], core_send.at[u], core_recv.at[u], core)
        total = wide(part_ref.at[2 * u + c]) + wide(core_in.at[u])
        sum_out[u] = total.astype(sum_out.dtype)
        start(remote(sum_out.at[u], y_in.at[j], y_send.at[j], y_recv.at[j], beside))
    for k in order:
        j = far(k)
        u = 2 * j + y
        arrived(core_in.at[u], core_send.at[u], core_recv.at[u], core)
        total = wide(part_ref.at[2 * u + c]) + wide(core_in.at[u])
        arrived(y_in.at[j], y_send.at[j], y_recv.at[j], beside)
        total = total + wide(y_in.at[j])
        if k != 0:
            sum_out[u] = total.astype(sum_out.dtype)
            start(
                remote(
                    sum_out.at[u],
                    z_in.at[z],
                    z_send.at[j],
                    z_recv.at[z],
                    {"seq": 4 * j + 2 * y + c},
                )
            )
    for k in range(1, depth):
        j = far(k)
        arrived(z_in.at[j], z_send.at[j], z_recv.at[j], core)
        total = total + wide(z_in.at[j])
    out_ref[...] = total.astype(out_ref.dtype)
    for copy in started:
        copy.wait_send()


def reduce_shards(parts, count):
    depth = count // 4
    block = parts.shape[1:]
    line, pairs = pltpu.SemaphoreType.DMA((depth,)), pltpu.SemaphoreType.DMA((2 * depth,))
    vmem = pl.BlockSpec(memory_space=pltpu.VMEM)
    return pl.pallas_call(
        functools.partial(reduce_kernel, depth),
        out_shape=jax.ShapeDtypeStruct(block, parts.dtype),
        in_specs=[vmem],
        out_specs=vmem,
        scratch_shapes=[
            pltpu.VMEM((2 * depth,) + block, parts.dtype),
            pltpu.VMEM((2 * depth,) + block, parts.dtype),
            pltpu.VMEM((depth,) + block, parts.dtype),
            pltpu.VMEM((depth,) + block, parts.dtype),
            pairs,
            pairs,
            line,
            line,
            line,
            line,
        ],
        compiler_params=pltpu.CompilerParams(collective_id=1, has_side_effects=True),
        name="reduce_shards",
    )(parts)


def swapped(array, axis, apart):
    return lax.ppermute(array, axis, [(i, i ^ 1 << apart) for i in range(lax.axis_size(axis))])


def body(
    queries,
    keys,
    values,
    out_grad,
    row_delta,
    layer_input,
    norm_gain,
    qkv_weight,
    block_order,
    block_mask,
    frame_owner,
    vision_features,
    post_gain,
    projector,
):
    tok_rows = queries.shape[0]
    half_len = tok_rows // 2
    my_index = lax.axis_index("seq")
    my_blocks = lax.dynamic_slice_in_dim(block_order, 2 * my_index, 2, 0)
    count = lax.axis_size("seq")
    kv_all, weight_all = gather(jnp.concatenate([keys, values], axis=1), qkv_weight, count)
    kv = kv_all.reshape(count * tok_rows, kv_all.shape[2])
    weight = weight_all.reshape(count * qkv_weight.shape[0], qkv_weight.shape[1])
    query_grad, kv_part = attention_grads(
        block_order, block_mask, queries, out_grad, row_delta, kv
    )
    kv_grad = reduce_shards(kv_part.reshape(kv_all.shape), count)
    head_grads = jnp.concatenate([query_grad, kv_grad], axis=1)
    norm_grad = jnp.dot(
        head_grads,
        weight.T,
        preferred_element_type=jnp.float32,
    ).astype(jnp.bfloat16)
    inputs = layer_input.astype(jnp.float32)
    inverse = lax.rsqrt(jnp.mean(inputs * inputs, axis=1, keepdims=True) + EPSILON)
    scaled = norm_grad.astype(jnp.float32) * norm_gain
    token_grad = (
        inverse * scaled - inputs * inverse**3 * jnp.mean(scaled * inputs, axis=1, keepdims=True)
    ).astype(jnp.bfloat16)
    frame_table = jnp.arange(frame_owner.shape[0], dtype=jnp.int32)
    my_frame = jnp.sum(jnp.where(frame_owner == my_index, frame_table, 0))
    keep_first = my_blocks[0] // 2 == my_frame
    kept_block = jnp.where(keep_first, my_blocks[0], my_blocks[1])
    leading = kept_block % 2 == 0
    halves = token_grad.reshape(2, half_len, token_grad.shape[1])
    kept = jnp.where(keep_first, halves[0], halves[1])
    sending = jnp.where(keep_first, halves[1], halves[0])
    received = swapped(sending, "seq", 0)
    frame_rows = jnp.where(
        leading,
        jnp.concatenate([kept, received], axis=0),
        jnp.concatenate([received, kept], axis=0),
    )
    post_grad = jnp.dot(frame_rows, projector.T, preferred_element_type=jnp.float32)
    features = vision_features[0].astype(jnp.float32)
    centered = features - jnp.mean(features, axis=1, keepdims=True)
    deviation = lax.rsqrt(jnp.mean(centered * centered, axis=1, keepdims=True) + EPSILON)
    normed = centered * deviation
    weighted = post_grad * post_gain
    encoder_grad = (
        deviation
        * (
            weighted
            - jnp.mean(weighted, axis=1, keepdims=True)
            - normed * jnp.mean(weighted * normed, axis=1, keepdims=True)
        )
    ).astype(jnp.bfloat16)
    return (token_grad, encoder_grad[None])


def solution(mesh):
    placed = (
        P(("batch", "seq"), None),
        P(("batch", "seq"), None),
        P(("batch", "seq"), None),
        P(("batch", "seq"), None),
        P(("batch", "seq"), None),
        P(("batch", "seq"), None),
        P(),
        P("seq", None),
        P("batch"),
        P("batch", None),
        P("batch"),
        P(("batch", "seq"), None, None),
        P(),
        P(),
    )
    return jax.shard_map(
        body,
        mesh=mesh,
        in_specs=placed,
        out_specs=(P(("batch", "seq"), None), P(("batch", "seq"), None, None)),
        check_vma=False,
    )
```

```python
import functools

import jax
import jax.numpy as jnp
from jax import lax
from jax.experimental import pallas as pl
from jax.experimental.pallas import tpu as pltpu
from jax.sharding import PartitionSpec as P

HQ = 14
KVH = 2
HD = 128
GROUP = HQ // KVH
CHUNK = 4
LOG2E = 1.4426950408889634


EPSILON = 1e-06
NEGATIVE = -1e30


def attention_kernel(
    order_ref,
    mask_ref,
    q_hbm,
    do_hbm,
    delta_ref,
    kv_hbm,
    dq_ref,
    dkv_ref,
    slots,
    scores,
    dq_acc,
    acc,
    q_ref,
    do_ref,
    kv_ref,
    load_sem,
):
    loads = [
        pltpu.make_async_copy(source, target, load_sem.at[i])
        for i, (source, target) in enumerate(
            ((kv_hbm, kv_ref), (q_hbm, q_ref), (do_hbm, do_ref))
        )
    ]
    for load in loads:
        load.start()
    me = lax.axis_index("seq")
    blocks = order_ref.shape[0]
    half = q_ref.shape[0] // 2
    lanes = delta_ref.shape[2]
    tall = CHUNK * half
    scaling = HD ** (-0.5)
    factor = scaling * LOG2E
    width = KVH * HD
    acc[...] = jnp.zeros_like(acc)

    row = lax.broadcasted_iota(jnp.int32, (tall, lanes), 0)
    query_at = lax.rem(lax.broadcasted_iota(jnp.int32, (tall, lanes), 1), half)
    ahead = (row < half) & (row > query_at)

    for load in loads:
        load.wait()

    for b in range(2):
        own = 2 * me + b
        query_block = order_ref[own]
        slots[0] = own

        def collect(slot, count):
            key_block = order_ref[slot]
            live = (mask_ref[query_block, key_block] == 1) & (key_block < query_block)
            slots[count] = slot
            return count + live.astype(jnp.int32)

        count = lax.fori_loop(0, blocks, collect, jnp.int32(1))
        for extra in range(CHUNK):
            slots[count + extra] = own
        chunks = (count + CHUNK - 1) // CHUNK

        for g in range(KVH):
            pad = jnp.zeros((lanes - GROUP * half, HD), jnp.bfloat16)

            def stacked(ref):
                parts = [
                    ref[b * half : (b + 1) * half, h * HD : (h + 1) * HD]
                    for h in range(g * GROUP, (g + 1) * GROUP)
                ]
                return jnp.concatenate(parts + [pad], axis=0)

            queries = stacked(q_ref)
            grads = stacked(do_ref)
            delta = delta_ref[2 * g + b]

            def key_rows(chunk, first_col):
                parts = [
                    kv_ref[
                        pl.ds(pl.multiple_of(slots[chunk * CHUNK + i] * half, half), half),
                        first_col : first_col + HD,
                    ]
                    for i in range(CHUNK)
                ]
                return jnp.concatenate(parts, axis=0)

            def score_pass(chunk, top):
                keys = key_rows(chunk, g * HD)
                score = lax.dot_general(
                    keys, queries, (((1,), (1,)), ((), ())), preferred_element_type=jnp.float32
                )
                limit = jnp.minimum((count - chunk * CHUNK) * half, tall)
                dead = (row >= limit) | (ahead & (chunk == 0))
                score = jnp.where(dead, NEGATIVE, score)
                scores[chunk] = score
                return jnp.maximum(top, jnp.max(score.reshape(tall // 8, 8, lanes), axis=0))

            top = lax.fori_loop(
                0, chunks, score_pass, jnp.full((8, lanes), NEGATIVE, jnp.float32)
            )
            top = jnp.max(top, axis=0, keepdims=True)

            def exp_pass(chunk, total):
                spread = jnp.exp2((scores[chunk] - top) * factor)
                scores[chunk] = spread
                return total + jnp.sum(spread.reshape(tall // 8, 8, lanes), axis=0)

            total = lax.fori_loop(0, chunks, exp_pass, jnp.zeros((8, lanes), jnp.float32))
            inverse = 1.0 / jnp.sum(total, axis=0, keepdims=True)
            dq_acc[...] = jnp.zeros_like(dq_acc)

            def grad_pass(chunk, carry):
                keys = key_rows(chunk, g * HD)
                vals = key_rows(chunk, width + g * HD)
                prob = scores[chunk] * inverse
                value_add = jnp.dot(
                    prob.astype(jnp.bfloat16), grads, preferred_element_type=jnp.float32
                )
                prob_grad = lax.dot_general(
                    vals, grads, (((1,), (1,)), ((), ())), preferred_element_type=jnp.float32
                )
                score_grad = (prob * (prob_grad - delta)).astype(jnp.bfloat16)
                key_add = (
                    jnp.dot(score_grad, queries, preferred_element_type=jnp.float32) * scaling
                )
                dq_acc[...] += lax.dot_general(
                    keys, score_grad, (((0,), (0,)), ((), ())), preferred_element_type=jnp.float32
                )
                for i in range(CHUNK):
                    here = pl.ds(pl.multiple_of(slots[chunk * CHUNK + i] * half, half), half)
                    part = slice(i * half, (i + 1) * half)
                    acc[here, g * HD : (g + 1) * HD] += key_add[part]
                    acc[here, width + g * HD : width + (g + 1) * HD] += value_add[part]
                return carry

            lax.fori_loop(0, chunks, grad_pass, 0)
            turned = (jnp.transpose(dq_acc[...]) * scaling).astype(jnp.bfloat16)
            for j in range(GROUP):
                h = g * GROUP + j
                dq_ref[b * half : (b + 1) * half, h * HD : (h + 1) * HD] = turned[
                    j * half : (j + 1) * half
                ]
    dkv_ref[...] = acc[...].astype(dkv_ref.dtype)


def attention_grads(order, mask, queries, out_grad, row_delta, kv):
    rows = queries.shape[0]
    half = rows // 2
    keys = kv.shape[0]
    lanes = -(-GROUP * half // 128) * 128
    blocks = order.shape[0]
    delta = jnp.transpose(row_delta.reshape(2, half, KVH, GROUP), (2, 0, 3, 1))
    delta = delta.reshape(2 * KVH, 1, GROUP * half)
    delta = jnp.pad(delta, ((0, 0), (0, 0), (0, lanes - GROUP * half)))
    max_chunks = -(-blocks // CHUNK)
    smem = pl.BlockSpec(memory_space=pltpu.SMEM)
    vmem = pl.BlockSpec(memory_space=pltpu.VMEM)
    anywhere = pl.BlockSpec(memory_space=pl.ANY)
    return pl.pallas_call(
        attention_kernel,
        out_shape=(
            jax.ShapeDtypeStruct((rows, HQ * HD), jnp.bfloat16),
            jax.ShapeDtypeStruct((keys, 2 * KVH * HD), jnp.bfloat16),
        ),
        in_specs=[smem, smem, anywhere, anywhere, vmem, anywhere],
        out_specs=(vmem, vmem),
        scratch_shapes=[
            pltpu.SMEM((blocks + CHUNK + 1,), jnp.int32),
            pltpu.VMEM((max_chunks, CHUNK * half, lanes), jnp.float32),
            pltpu.VMEM((HD, lanes), jnp.float32),
            pltpu.VMEM((keys, 2 * KVH * HD), jnp.float32),
            pltpu.VMEM(queries.shape, queries.dtype),
            pltpu.VMEM(out_grad.shape, out_grad.dtype),
            pltpu.VMEM(kv.shape, kv.dtype),
            pltpu.SemaphoreType.DMA((3,)),
        ],
        cost_estimate=pl.CostEstimate(
            flops=5 * rows * keys * HQ * HD,
            bytes_accessed=4 * keys * KVH * HD * 2 + 3 * rows * HQ * HD * 2,
            transcendentals=rows * keys * HQ // 2,
        ),
        compiler_params=pltpu.CompilerParams(vmem_limit_bytes=67043328),
        name="attention_grads",
    )(order, mask, queries, out_grad, delta, kv)


MESH = pl.DeviceIdType.MESH


def remote(src, dst, send_sem, recv_sem, device):
    return pltpu.make_async_remote_copy(
        src_ref=src,
        dst_ref=dst,
        send_sem=send_sem,
        recv_sem=recv_sem,
        device_id=device,
        device_id_type=MESH,
    )


def when(condition, action):
    if condition is None:
        action()
    else:
        pl.when(condition)(action)


def places():
    me = lax.axis_index("seq")
    x = lax.rem(lax.axis_index("batch"), 2)
    z, y, c = me // 4, lax.rem(me // 2, 2), lax.rem(me, 2)
    return me, x, z, y, c


def gather_kernel(
    depth,
    k_ref,
    v_ref,
    w_ref,
    kv_all,
    w_all,
    kv_own,
    w_own,
    own_sem,
    kv_recv,
    kv_core_recv,
    kv_up,
    kv_down,
    kv_y,
    kv_core,
    w_recv,
    w_x_recv,
    w_core_recv,
    w_up,
    w_down,
    w_y,
    w_x,
    w_core,
):
    me, x, z, y, c = places()
    rows = w_ref.shape[0]
    width = k_ref.shape[1]
    part = 5 * (rows // 16) // 14 * 16
    up, down = {"seq": me + 4}, {"seq": me - 4}
    beside, core = {"seq": me + 2 - 4 * y}, {"seq": me + 1 - 2 * c}
    across = {"batch": lax.axis_index("batch") + 1 - 2 * x}
    has_up, has_down = z < depth - 1, z > 0

    loads = [
        pltpu.make_async_copy(k_ref, kv_own.at[:, 0:width], own_sem.at[0]),
        pltpu.make_async_copy(v_ref, kv_own.at[:, width : 2 * width], own_sem.at[1]),
        pltpu.make_async_copy(w_ref, w_own, own_sem.at[2]),
    ]
    for load in loads:
        load.start()
    barrier = pltpu.get_barrier_semaphore()
    for peer, present in (
        (up, has_up),
        (down, has_down),
        (beside, None),
        (core, None),
        (across, None),
    ):
        when(
            present,
            lambda peer=peer: pl.semaphore_signal(
                barrier, inc=1, device_id=peer, device_id_type=MESH
            ),
        )
    pl.semaphore_wait(barrier, 3 + has_up.astype(jnp.int32) + has_down.astype(jnp.int32))
    for load in loads:
        load.wait()

    started = []

    def start(copy, condition=None):
        when(condition, copy.start)
        started.append((condition, copy))

    def both(first, second):
        return second if first is None else jnp.logical_and(first, second)

    def line(step):
        if step == 0:
            return [(z, None, None)]
        return [(z - step, z - step >= 0, True), (z + step, z + step < depth, False)]

    def safe(j):
        return jnp.clip(j, 0, depth - 1)

    def slot(j, side):
        return 2 * j + side

    def arrived(ref, semaphore, condition=None):
        when(condition, remote(ref, ref, own_sem.at[3], semaphore, core).wait_recv)

    own_kv = pltpu.make_async_copy(kv_own, kv_all.at[me], own_sem.at[4])
    own_w = pltpu.make_async_copy(w_own, w_all.at[me], own_sem.at[5])

    def kv_at(u):
        return kv_all.at[2 * u + c]

    def kv_core_pass(src, u, condition):
        start(remote(src, kv_at(u), kv_core.at[u], kv_core_recv.at[u], core), condition)

    def kv_pass(j, condition, upward):
        u = slot(j, y)
        src = kv_own if upward is None else kv_at(u)
        if upward is not False:
            start(remote(src, kv_at(u), kv_up.at[j], kv_recv.at[u], up), both(condition, has_up))
        if upward is not True:
            start(
                remote(src, kv_at(u), kv_down.at[j], kv_recv.at[u], down),
                both(condition, has_down),
            )
        start(remote(src, kv_at(u), kv_y.at[j], kv_recv.at[u], beside), condition)
        kv_core_pass(src, u, condition)

    spans = [
        pl.ds(pl.multiple_of(x * (rows - part), 16), part),
        pl.ds(part, rows - 2 * part),
        pl.ds(pl.multiple_of((1 - x) * (rows - part), 16), part),
    ]

    def w_at(u, r):
        return w_all.at[2 * u + c, spans[r]]

    def w_core_pass(src, u, r, condition):
        start(remote(src, w_at(u, r), w_core.at[r, u], w_core_recv.at[r, u], core), condition)

    def w_share(u, r, condition):
        if r == 0:
            start(
                remote(w_at(u, 0), w_at(u, 0), w_x.at[u], w_x_recv.at[u], across), condition
            )
        w_core_pass(w_at(u, r), u, r, condition)

    def w_pass(j, r, condition, upward):
        u = slot(j, y)
        src = w_own.at[spans[r]] if upward is None else w_at(u, r)
        dst = w_at(u, r)
        if upward is not False:
            start(remote(src, dst, w_up.at[r, j], w_recv.at[r, u], up), both(condition, has_up))
        if upward is not True:
            start(
                remote(src, dst, w_down.at[r, j], w_recv.at[r, u], down),
                both(condition, has_down),
            )
        start(remote(src, dst, w_y.at[r, j], w_recv.at[r, u], beside), condition)

    kv_pass(z, None, None)
    for r in (0, 1):
        w_pass(z, r, None, None)
    for r in (0, 1, 2):
        w_core_pass(w_own.at[spans[r]], slot(z, y), r, None)
    own_kv.start()
    own_w.start()

    waiting = []
    for step in range(1, depth + 1):
        shared = []
        ahead = [(safe(j), present, upward) for j, present, upward in line(step)]
        ahead = ahead if step < depth else []
        aside = [(slot(safe(j), 1 - y), present) for j, present, _ in line(step - 1)]
        for j, condition, upward in ahead:
            arrived(kv_at(slot(j, y)), kv_recv.at[slot(j, y)], condition)
            kv_pass(j, condition, upward)
        for u, condition in aside:
            arrived(kv_at(u), kv_recv.at[u], condition)
            kv_core_pass(kv_at(u), u, condition)
        for r in (0, 1):
            for j, condition, upward in ahead:
                u = slot(j, y)
                arrived(w_at(u, r), w_recv.at[r, u], condition)
                w_pass(j, r, condition, upward)
                w_share(u, r, condition)
            for u, condition in aside:
                arrived(w_at(u, r), w_recv.at[r, u], condition)
                w_share(u, r, condition)
        shared = [(slot(j, y), condition) for j, condition, _ in ahead] + aside
        for u, condition in waiting:
            arrived(w_at(u, 2), w_x_recv.at[u], condition)
            w_core_pass(w_at(u, 2), u, 2, condition)
        waiting = shared
    for u, condition in waiting:
        arrived(w_at(u, 2), w_x_recv.at[u], condition)
        w_core_pass(w_at(u, 2), u, 2, condition)

    for u in range(2 * depth):
        from_core = 2 * u + 1 - c
        arrived(kv_all.at[from_core], kv_core_recv.at[u])
        for r in (0, 1, 2):
            arrived(w_all.at[from_core, spans[r]], w_core_recv.at[r, u])
    for condition, copy in started:
        when(condition, copy.wait_send)
    own_kv.wait()
    own_w.wait()


def gather(keys, values, weight, count):
    depth = count // 4
    kv_shape = (keys.shape[0], 2 * keys.shape[1])

    def sems(*shape):
        return pltpu.SemaphoreType.DMA(shape)

    pairs = 2 * depth
    anywhere = pl.BlockSpec(memory_space=pl.ANY)
    return pl.pallas_call(
        functools.partial(gather_kernel, depth),
        out_shape=(
            jax.ShapeDtypeStruct((count,) + kv_shape, keys.dtype),
            jax.ShapeDtypeStruct((count,) + weight.shape, weight.dtype),
        ),
        in_specs=[anywhere, anywhere, anywhere],
        out_specs=(anywhere, anywhere),
        scratch_shapes=[
            pltpu.VMEM(kv_shape, keys.dtype),
            pltpu.VMEM(weight.shape, weight.dtype),
            sems(6),
            sems(pairs),
            sems(pairs),
            sems(depth),
            sems(depth),
            sems(depth),
            sems(pairs),
            sems(2, pairs),
            sems(pairs),
            sems(3, pairs),
            sems(2, depth),
            sems(2, depth),
            sems(2, depth),
            sems(pairs),
            sems(3, pairs),
        ],
        compiler_params=pltpu.CompilerParams(collective_id=0, has_side_effects=True),
        name="gather",
    )(keys, values, weight)


def reduce_kernel(
    depth,
    part_ref,
    out_ref,
    core_in,
    sum_out,
    y_in,
    z_in,
    core_send,
    core_recv,
    y_send,
    y_recv,
    z_send,
    z_recv,
):
    me, x, z, y, c = places()
    beside, core = {"seq": me + 2 - 4 * y}, {"seq": me + 1 - 2 * c}

    def far(k):
        return lax.rem(z + k, depth)

    barrier = pltpu.get_barrier_semaphore()
    peers = [beside, core] + [{"seq": 4 * far(k) + 2 * y + c} for k in range(1, depth)]
    for peer in peers:
        pl.semaphore_signal(barrier, inc=1, device_id=peer, device_id_type=MESH)
    pl.semaphore_wait(barrier, len(peers))

    def wide(ref):
        return ref[...].astype(jnp.float32)

    order = list(range(1, depth)) + [0]
    started = []

    def start(copy):
        copy.start()
        started.append(copy)

    core_copies, y_copies = {}, {}
    for side in (1, 0):
        for k in order:
            u = 2 * far(k) + (y if side == 0 else 1 - y)
            copy = remote(
                part_ref.at[2 * u + 1 - c], core_in.at[u], core_send.at[u], core_recv.at[u], core
            )
            start(copy)
            core_copies[side, k] = (copy, u)

    def arrived(ref, send_semaphore, semaphore, device):
        remote(ref, ref, send_semaphore, semaphore, device).wait_recv()

    for k in order:
        j = far(k)
        u = 2 * j + 1 - y
        arrived(core_in.at[u], core_send.at[u], core_recv.at[u], core)
        total = wide(part_ref.at[2 * u + c]) + wide(core_in.at[u])
        sum_out[u] = total.astype(sum_out.dtype)
        start(remote(sum_out.at[u], y_in.at[j], y_send.at[j], y_recv.at[j], beside))
    for k in order:
        j = far(k)
        u = 2 * j + y
        arrived(core_in.at[u], core_send.at[u], core_recv.at[u], core)
        total = wide(part_ref.at[2 * u + c]) + wide(core_in.at[u])
        arrived(y_in.at[j], y_send.at[j], y_recv.at[j], beside)
        total = total + wide(y_in.at[j])
        if k != 0:
            sum_out[u] = total.astype(sum_out.dtype)
            start(
                remote(
                    sum_out.at[u],
                    z_in.at[z],
                    z_send.at[j],
                    z_recv.at[z],
                    {"seq": 4 * j + 2 * y + c},
                )
            )
    for k in range(1, depth):
        j = far(k)
        arrived(z_in.at[j], z_send.at[j], z_recv.at[j], core)
        total = total + wide(z_in.at[j])
    out_ref[...] = total.astype(out_ref.dtype)
    for copy in started:
        copy.wait_send()


def reduce_shards(parts, count):
    depth = count // 4
    block = parts.shape[1:]
    line, pairs = pltpu.SemaphoreType.DMA((depth,)), pltpu.SemaphoreType.DMA((2 * depth,))
    vmem = pl.BlockSpec(memory_space=pltpu.VMEM)
    return pl.pallas_call(
        functools.partial(reduce_kernel, depth),
        out_shape=jax.ShapeDtypeStruct(block, parts.dtype),
        in_specs=[vmem],
        out_specs=vmem,
        scratch_shapes=[
            pltpu.VMEM((2 * depth,) + block, parts.dtype),
            pltpu.VMEM((2 * depth,) + block, parts.dtype),
            pltpu.VMEM((depth,) + block, parts.dtype),
            pltpu.VMEM((depth,) + block, parts.dtype),
            pairs,
            pairs,
            line,
            line,
            line,
            line,
        ],
        compiler_params=pltpu.CompilerParams(collective_id=1, has_side_effects=True),
        name="reduce_shards",
    )(parts)


def swapped(array, axis, apart):
    return lax.ppermute(array, axis, [(i, i ^ 1 << apart) for i in range(lax.axis_size(axis))])


def body(
    queries,
    keys,
    values,
    out_grad,
    row_delta,
    layer_input,
    norm_gain,
    qkv_weight,
    block_order,
    block_mask,
    frame_owner,
    vision_features,
    post_gain,
    projector,
):
    tok_rows = queries.shape[0]
    half_len = tok_rows // 2
    my_index = lax.axis_index("seq")
    my_blocks = lax.dynamic_slice_in_dim(block_order, 2 * my_index, 2, 0)
    count = lax.axis_size("seq")
    kv_all, weight_all = gather(keys, values, qkv_weight, count)
    kv = kv_all.reshape(count * tok_rows, kv_all.shape[2])
    weight = weight_all.reshape(count * qkv_weight.shape[0], qkv_weight.shape[1])
    query_grad, kv_part = attention_grads(
        block_order, block_mask, queries, out_grad, row_delta, kv
    )
    kv_grad = reduce_shards(kv_part.reshape(kv_all.shape), count)
    head_grads = jnp.concatenate([query_grad, kv_grad], axis=1)
    norm_grad = jnp.dot(
        head_grads,
        weight.T,
        preferred_element_type=jnp.float32,
    ).astype(jnp.bfloat16)
    inputs = layer_input.astype(jnp.float32)
    inverse = lax.rsqrt(jnp.mean(inputs * inputs, axis=1, keepdims=True) + EPSILON)
    scaled = norm_grad.astype(jnp.float32) * norm_gain
    token_grad = (
        inverse * scaled - inputs * inverse**3 * jnp.mean(scaled * inputs, axis=1, keepdims=True)
    ).astype(jnp.bfloat16)
    frame_table = jnp.arange(frame_owner.shape[0], dtype=jnp.int32)
    my_frame = jnp.sum(jnp.where(frame_owner == my_index, frame_table, 0))
    keep_first = my_blocks[0] // 2 == my_frame
    kept_block = jnp.where(keep_first, my_blocks[0], my_blocks[1])
    leading = kept_block % 2 == 0
    halves = token_grad.reshape(2, half_len, token_grad.shape[1])
    kept = jnp.where(keep_first, halves[0], halves[1])
    sending = jnp.where(keep_first, halves[1], halves[0])
    received = swapped(sending, "seq", 0)
    frame_rows = jnp.where(
        leading,
        jnp.concatenate([kept, received], axis=0),
        jnp.concatenate([received, kept], axis=0),
    )
    post_grad = jnp.dot(frame_rows, projector.T, preferred_element_type=jnp.float32)
    features = vision_features[0].astype(jnp.float32)
    centered = features - jnp.mean(features, axis=1, keepdims=True)
    deviation = lax.rsqrt(jnp.mean(centered * centered, axis=1, keepdims=True) + EPSILON)
    normed = centered * deviation
    weighted = post_grad * post_gain
    encoder_grad = (
        deviation
        * (
            weighted
            - jnp.mean(weighted, axis=1, keepdims=True)
            - normed * jnp.mean(weighted * normed, axis=1, keepdims=True)
        )
    ).astype(jnp.bfloat16)
    return (token_grad, encoder_grad[None])


def solution(mesh):
    placed = (
        P(("batch", "seq"), None),
        P(("batch", "seq"), None),
        P(("batch", "seq"), None),
        P(("batch", "seq"), None),
        P(("batch", "seq"), None),
        P(("batch", "seq"), None),
        P(),
        P("seq", None),
        P("batch"),
        P("batch", None),
        P("batch"),
        P(("batch", "seq"), None, None),
        P(),
        P(),
    )
    return jax.shard_map(
        body,
        mesh=mesh,
        in_specs=placed,
        out_specs=(P(("batch", "seq"), None), P(("batch", "seq"), None, None)),
        check_vma=False,
    )
```
